32 devices in a mesh: row: 4 (over z), col: 4 (over y, x), layer: 2 (over core).
Axes of the slice: x: 2, y: 2, z: 4, core: 2. Of those that a mesh axis runs over, the one named last changes fastest.
Arguments:
- basis: float32 [4096, 4096], P('row', 'col'), may hold values from -1 to 1, as said below
- basis_grad: float32 [4096, 4096], P('row', 'col'), may hold values from -768 to 768
- value_grad: float32 [4096], replicated, may hold values from -384 to 384
- ranks: int32 [4096], replicated, may hold values from 0 to 4095, each once
- offsets: int32 [4096], replicated, may hold values from 0 to 3
Outputs:
- grad_matrix: float32 [4096, 4096], P(('row', 'layer'), 'col')
The draws below stay inside these ranges and needn't reach their ends.
Inputs may be any that keep to these rules, and one draw needn't show every extreme that they name: The columns of basis are orthonormal. ranks holds every number of 0 to 4095 once, so eigenvalues of different indices differ by 1 or more.
All inputs are finite; a program needn't handle non-finite values.
Results may differ from the reference program's by a relative error of at most 0.000098.
Values sent between devices are 32-bit elements; how exact they have to be, the bound alone decides.
A program may use at most 128 MiB of HBM per device.

```python
import jax
import jax.numpy as jnp
from jax import lax

N = 4096


def draw_basis(key, part):
    source = jax.random.normal(key, (N, N), jnp.float32)
    factor, upper = jnp.linalg.qr(source)
    signs = jnp.where(jnp.diagonal(upper) < 0, -1.0, 1.0)
    return (factor * signs[None, :]).astype(jnp.float32)


def with_ends(values, key, low, largest):
    longest = values.shape.index(max(values.shape))
    spots = []
    for shift in (0, 1):
        where = [jax.random.randint(jax.random.fold_in(key, axis), (), 0, length) for axis, length in enumerate(values.shape)]
        where[longest] = (where[longest] + shift) % values.shape[longest]
        spots.append(tuple(where))
    return values.at[spots[0]].set(low).at[spots[1]].set(largest)


def level_of(key, shape, shards, smallest, high):
    gain = 1.0
    for axis_at, blocks in shards:
        draws = jax.random.uniform(jax.random.fold_in(jax.random.fold_in(key, 6), axis_at), (blocks,), jnp.float32, smallest / len(shards), high / len(shards))
        gain = gain * jnp.repeat(jnp.exp(draws), shape[axis_at] // blocks).reshape((-1,) + (1,) * (len(shape) - 1 - axis_at))
    return gain


def noise(key, extent, width, most, shards=(), kind=jnp.bfloat16):
    drawn = jax.random.normal(key, extent, jnp.float32) * width
    if len(shards) > 0:
        drawn = level_of(key, extent, shards, -0.22, 0.18) * drawn
    return jnp.clip(drawn, min=-most, max=most).astype(kind)


def setup_inputs(seed: int = 0) -> dict:
    key_of = jax.random.split(jax.random.key(seed), 6)
    basis = draw_basis(jax.random.fold_in(key_of[5], 71), 0)
    basis_grad = noise(key_of[1], (N, N), (2 * N ** 0.5), 768.0, ((0, 4), (1, 4)), jnp.float32)
    value_grad = noise(key_of[2], (N,), (N ** 0.5), 384.0, (), jnp.float32)
    ranks = jax.random.permutation(key_of[3], N).astype(jnp.int32)
    offsets = with_ends(jax.random.randint(key_of[4], (N,), 0, 4), jax.random.fold_in(key_of[4], 1), 0, 3).astype(jnp.int32)
    return dict(basis=basis, basis_grad=basis_grad, value_grad=value_grad, ranks=ranks, offsets=offsets)


def reference(basis, basis_grad, value_grad, ranks, offsets):
    highest = lax.Precision.HIGHEST
    eigen = 4.0 * ranks.astype(jnp.float32) + offsets.astype(jnp.float32)
    inner = jnp.dot(basis.T.astype(jnp.float32), basis_grad.astype(jnp.float32), precision=highest, preferred_element_type=jnp.float32)
    index = jnp.arange(N, dtype=jnp.int32)
    on_diagonal = index[:, None] == index[None, :]
    spacing = eigen[None, :] - eigen[:, None]
    scaled = jnp.where(on_diagonal, value_grad[None, :], inner / jnp.where(on_diagonal, jnp.float32(1.0), spacing))
    left_prod = jnp.dot(basis.astype(jnp.float32), scaled.astype(jnp.float32), precision=highest, preferred_element_type=jnp.float32)
    return jnp.dot(left_prod.astype(jnp.float32), basis.T.astype(jnp.float32), precision=highest, preferred_element_type=jnp.float32)
```

```python
import jax
import jax.numpy as jnp
from jax import lax
from jax.sharding import PartitionSpec as P


def dot(a, b, dims):
    return lax.dot_general(
        a, b, (dims, ((), ())), precision=lax.Precision.HIGH, preferred_element_type=jnp.float32
    )


def flip(v, axis, q):
    n = lax.axis_size(axis)
    return lax.ppermute(v, axis, [(i, i ^ q) for i in range(n)])


def shift(v, axis, d):
    if d == 0:
        return v
    n = lax.axis_size(axis)
    return lax.ppermute(v, axis, [(i, (i + d) % n) for i in range(n)])


def gather_begin(v):
    n = lax.axis_size("col")
    if n != 4:
        return [flip(v, "col", q) for q in range(1, n)]
    half = v.shape[0] // 2
    a, b = v[:half], v[half:]
    return [flip(a, "col", 1), flip(b, "col", 2), flip(a, "col", 2), flip(b, "col", 1)]


def gather_end(v, first):
    if lax.axis_size("col") != 4:
        return [v] + first
    a1, b2, a2, b1 = first
    a3, b3 = flip(a1, "col", 2), flip(b2, "col", 1)
    return [v] + [jnp.concatenate(pair) for pair in ((a1, b1), (a2, b2), (a3, b3))]


def scatter_cols(part, rows):
    n = lax.axis_size("col")
    order = (3, 1, 2, 0) if n == 4 else tuple(range(1, n)) + (0,)
    term = {q: lax.optimization_barrier(part(q)) for q in order}
    if n != 4:
        moved = [flip(term[q], "col", q) for q in range(1, n)]
        total = term[0]
        for v in moved:
            total = total + v
        return total, moved[0]
    half = rows // 2
    pa = {q: v[:half] for q, v in term.items()}
    pb = {q: v[half:] for q, v in term.items()}
    moved = flip(pa[3], "col", 1)
    a2 = pa[2] + moved
    b1 = pb[1] + flip(pb[3], "col", 2)
    a0 = pa[0] + flip(pa[1], "col", 1)
    b0 = pb[0] + flip(pb[2], "col", 2)
    return jnp.concatenate([a0 + flip(a2, "col", 2), b0 + flip(b1, "col", 1)]), moved


def swap_layers(mine, axis):
    if lax.axis_size("layer") != 2:
        return lax.all_gather(mine, "layer", axis=axis, tiled=True)
    other = flip(mine, "layer", 1)
    first = lax.axis_index("layer") == 0
    return jnp.concatenate([jnp.where(first, mine, other), jnp.where(first, other, mine)], axis=axis)


def on_device(basis, basis_grad, value_grad, ranks, offsets):
    rows_blk, cols_blk = basis.shape
    nr, nc, nl = (lax.axis_size(a) for a in ("row", "col", "layer"))
    row_id, col_id, layer_id = (lax.axis_index(a) for a in ("row", "col", "layer"))
    width = cols_blk // (nr * nl)
    half = rows_blk // nl

    pieces = [None] * nr
    for d in range(nr):
        begin = (lax.rem(row_id + d, nr) * nl + layer_id) * width
        piece = lax.dynamic_slice_in_dim(basis_grad, begin, width, 1)
        pieces[(nr - d) % nr] = shift(piece, "row", d)

    mine = lax.dynamic_slice_in_dim(basis, layer_id * half, half, 0)
    up, down = [mine], [mine]
    for s in range(1, nr):
        up.append(lax.ppermute(up[-1], "row", [(i, i + 1) for i in range(s - 1, nr - 1)]))
        down.append(lax.ppermute(down[-1], "row", [(i, i - 1) for i in range(1, nr - s + 1)]))
        if s == 1:
            up[1], down[1], pieces = lax.optimization_barrier((up[1], down[1], pieces))
            pieces = jnp.concatenate(pieces)
            begun = gather_begin(pieces)
        if s == 2:
            up[2], down[2], begun = lax.optimization_barrier((up[2], down[2], begun))
    cotangent = jnp.concatenate(gather_end(pieces, begun), axis=1).reshape(nr, rows_blk, nc * width)
    vectors = [basis]
    for e in range(1, nr):
        block = jnp.where(row_id + e < nr, down[e], up[nr - e])
        vectors.append(swap_layers(block, 0))

    inner = dot(vectors[0], cotangent[0], ((0,), (0,)))
    for e in sorted(range(1, nr), key=lambda e: min(e, nr - e)):
        inner = inner + dot(vectors[e], cotangent[e], ((0,), (0,)))

    eigen = 4.0 * ranks.astype(jnp.float32) + offsets.astype(jnp.float32)
    place = row_id * nl + layer_id

    def columns(v):
        mine = lax.dynamic_index_in_dim(v.reshape(nc, nr * nl, width), place, 1, keepdims=False)
        return jnp.concatenate([lax.dynamic_index_in_dim(mine, col_id ^ q, 0, keepdims=False) for q in range(nc)])

    row_index = col_id * cols_blk + jnp.arange(cols_blk, dtype=jnp.int32)
    col_index = columns(jnp.arange(nc * cols_blk, dtype=jnp.int32))
    eigen_rows = lax.dynamic_slice_in_dim(eigen, col_id * cols_blk, cols_blk, 0)
    on_diagonal = row_index[:, None] == col_index[None, :]
    spacing = columns(eigen)[None, :] - eigen_rows[:, None]
    scaled = jnp.where(
        on_diagonal, columns(value_grad)[None, :], inner / jnp.where(on_diagonal, jnp.float32(1.0), spacing)
    )

    arrived = [None] * nr
    order = sorted(range(nr), key=lambda e: -min(e, nr - e))
    groups = [g for g in (order[:nr // 2 - 1], order[nr // 2 - 1:nr - 1], order[nr - 1:]) if g]
    factor = scaled
    for group in groups:
        product = dot(jnp.concatenate([vectors[e] for e in group]), factor, ((1,), (0,)))
        product = lax.optimization_barrier(product)
        summed, first = scatter_cols(lambda q: product[:, q * width:(q + 1) * width], product.shape[0])
        factor, first = lax.optimization_barrier((factor, first))
        for i, e in enumerate(group):
            arrived[e] = shift(summed[i * rows_blk:(i + 1) * rows_blk], "row", e)
    own = []
    for e in range(nr):
        keep = lax.dynamic_slice_in_dim(arrived[e], layer_id * half, half, 0)
        if nl == 1:
            own.append(keep)
            continue
        give = lax.dynamic_slice_in_dim(arrived[e], (1 - layer_id) * half, half, 0)
        other = flip(give, "layer", 1)
        first = layer_id == 0
        own.append(jnp.concatenate([jnp.where(first, keep, other), jnp.where(first, other, keep)], axis=1))
    own = jnp.stack(own)
    left = jnp.concatenate(
        [lax.dynamic_index_in_dim(own, lax.rem(row_id - r + nr, nr), 0, keepdims=False) for r in range(nr)], axis=1
    )

    stack = jnp.stack(vectors)

    def grad_part(q):
        e = lax.rem((col_id ^ q) - row_id + nr, nr)
        block = lax.dynamic_index_in_dim(stack, e, 0, keepdims=False)
        return dot(left, block, ((1,), (1,)))

    return scatter_cols(grad_part, half)[0]


def solution(mesh):
    placed = (P("row", "col"), P("row", "col"), P(), P(), P())
    return jax.shard_map(
        on_device, mesh=mesh, in_specs=placed, out_specs=P(("row", "layer"), "col"), check_vma=False
    )
```
